128 devices in a mesh: vocab: 32 (over x, z, core), group: 4 (over y).
Axes of the slice: x: 4, y: 4, z: 4, core: 2. Of those that a mesh axis runs over, the one named last changes fastest.
Arguments:
- hidden_states: bfloat16 [2048, 4096], P(('group', 'vocab')), parts along dimension 0, may hold values from -32 to 32
- head_weight: bfloat16 [4096, 77824], P(None, 'vocab'), may hold values from -1 to 1
- pick_index: int32 [2048, 64], P('group'), parts along dimension 0, may hold values from 0 to 77823, as said below
- owner_order: int32 [2048], P('group'), parts along dimension 0, may hold values from 0 to 511, each once
Outputs:
- token_logprobs: float32 [2048, 64], P(('group', 'vocab')), parts along dimension 0
- token_logtotal: float32 [2048], P(('group', 'vocab')), parts along dimension 0
The draws below stay inside these ranges and needn't reach their ends.
There are 4 independent parts, one for each index of `group`. The reference program is written for one: setup_inputs(seed, part) draws one part's arguments, and reference() takes and returns one part's arrays. A program takes and returns all parts, laid end to end along the dimension named above; an argument that names none is the same for every part. Nothing has to cross between parts.
Inputs may be any that keep to these rules, and one draw needn't show every extreme that they name: `pick_index`: each row holds 64 distinct vocabulary entries. `owner_order`: each token appears once.
All inputs are finite; a program needn't handle non-finite values.
Results may differ from the reference program's by a relative error of at most 0.0003.
Values may be sent and summed in bfloat16 or wider, within the bound.
A program may use at most 128 MiB of HBM per device.

```python
import math
import jax
import jax.numpy as jnp

D = 4096
K = 64
TOKENS = 512
VOCAB = 77824


def weight_column(key, column):
    column_key = jax.random.fold_in(jax.random.fold_in(key, 7), column)
    values = jnp.clip(jax.random.normal(column_key, (D,), jnp.float32), -6.0, 6.0)
    factor = jnp.exp(jax.random.uniform(jax.random.fold_in(column_key, 1), (), jnp.float32, math.log(0.7), math.log(1.4)))
    position = column.astype(jnp.float32) / VOCAB
    scale = 3.0 * jnp.exp(0.13 * position) * factor
    return values * scale / math.sqrt(D)


def draw_head_weight(key, part):
    columns = jax.vmap(lambda column: weight_column(key, column))(jnp.arange(VOCAB, dtype=jnp.int32))
    result = columns.T
    return jnp.clip(result, -1.0, 1.0).astype(jnp.bfloat16)


def draw_hidden_states(key, part):
    base_key = jax.random.fold_in(key, 11)
    result = jnp.clip(jax.random.normal(base_key, (TOKENS, D), jnp.float32), -6.0, 6.0)
    return jnp.clip(result, -32.0, 32.0).astype(jnp.bfloat16)


def draw_pick_index(key, part):
    base_key = jax.random.fold_in(key, 21)
    raw_draw = jax.random.randint(base_key, (TOKENS, K), 0, VOCAB - K + 1)
    spread = jnp.sort(raw_draw, axis=1) + jnp.arange(K, dtype=jnp.int32)[None, :]
    scores = jax.random.randint(jax.random.fold_in(base_key, 1), (TOKENS, K), 0, 1 << 20) * K + jnp.arange(K, dtype=jnp.int32)[None, :]
    shuffle = jnp.argsort(scores, axis=1, stable=True)
    return jnp.take_along_axis(spread, shuffle, axis=1).astype(jnp.int32)


def setup_inputs(seed: int = 0, part: int = 0) -> dict:
    streams_of = jax.random.split(jax.random.key(seed), 5)
    own_keys = jax.random.split(jax.random.fold_in(streams_of[4], part), 5)
    hidden_states = draw_hidden_states(jax.random.fold_in(jax.random.fold_in(streams_of[4], part), 71), part)
    head_weight = draw_head_weight(jax.random.fold_in(streams_of[4], 71), part)
    pick_index = draw_pick_index(jax.random.fold_in(jax.random.fold_in(streams_of[4], part), 71), part)
    owner_order = jax.random.permutation(own_keys[3], TOKENS).astype(jnp.int32)
    return {"hidden_states": hidden_states, "head_weight": head_weight, "pick_index": pick_index, "owner_order": owner_order}


def reference(hidden_states, head_weight, pick_index, owner_order):
    logits = jnp.dot(hidden_states, head_weight, preferred_element_type=jnp.float32)
    row_max = jnp.max(logits, axis=1)
    log_total = row_max + jnp.log(jnp.sum(jnp.exp(logits - row_max[:, None]), axis=1))
    picked = jnp.take_along_axis(logits, pick_index, axis=1) - log_total[:, None]
    return picked[owner_order], log_total[owner_order]
```

```python
import functools

import jax
import jax.numpy as jnp
from jax import lax
from jax.experimental import pallas as pl
from jax.experimental.pallas import tpu as pltpu
from jax.sharding import PartitionSpec as P

MESH = pl.DeviceIdType.MESH
SIDE = 4
SHARDS = 2 * SIDE * SIDE
LANES = 128
TILE = 512
BLOCKS = 4
PLACE = {
    (0, 0): (0, 0), (3, 0): (0, 1), (1, 0): (0, 2), (0, 1): (0, 3),
    (0, 3): (1, 0), (2, 0): (1, 1), (3, 1): (1, 2), (3, 3): (1, 3),
    (1, 1): (2, 0), (1, 3): (2, 1), (2, 1): (2, 2), (2, 3): (2, 3),
    (0, 2): (3, 0), (3, 2): (3, 1), (1, 2): (3, 2), (2, 2): (3, 3),
}
HALVED = ((2, 0), (0, 2), (3, 2), (1, 2), (2, 2))
WHOLE = tuple(rel for rel in PLACE if rel not in HALVED and rel != (0, 0))
ARRIVALS = [(rel, None) for rel in WHOLE] + [(rel, half) for rel in HALVED for half in (0, 1)]
RECV = {key: number for number, key in enumerate(ARRIVALS)}
SENDS = 40


def flat(x, z, core):
    return ((x % SIDE) * SIDE + z % SIDE) * 2 + core


def kernel(
    x_ref, w_ref, pick_ref, order_ref, logp_ref, total_ref,
    hidden, weight, logits, top, mass, found, low, high, pieces, perm, outbox, inbox,
    own_sem, weight_sem, send_sem, recv_sem, pair_sem, out_sem, in_sem,
):
    rows, depth = x_ref.shape
    width = w_ref.shape[1]
    tokens, picks = pick_ref.shape
    half_depth = depth // 2
    chunk_rows = 2 * BLOCKS * rows
    tiles = [(start, min(TILE, width - start)) for start in range(0, width, TILE)]

    me = lax.axis_index("vocab")
    core = me % 2
    x = me // 2 // SIDE
    z = me // 2 % SIDE
    pair = me + 1 - 2 * core

    def at(da, db, kind):
        return (1 - kind) * flat(x + da, z + db, kind) + kind * flat(x + db, z + da, kind)

    first_up, first_down = at(1, 0, core), at(3, 0, core)
    second_up, second_down = at(0, 1, core), at(0, 3, core)

    def block(rel, half=None, other=0):
        chunk, slot = PLACE[rel]
        row = (slot + BLOCKS * other) * rows
        if half is None:
            return hidden.at[chunk, pl.ds(row, rows), :]
        return hidden.at[chunk, pl.ds(row, rows), pl.ds(half * half_depth, half_depth)]

    own_copy = pltpu.make_async_copy(x_ref, block((0, 0)), own_sem)
    own_copy.start()
    weight_copies = []
    for number, (start, size) in enumerate(tiles):
        copy = pltpu.make_async_copy(
            w_ref.at[:, pl.ds(start, size)], weight.at[:, pl.ds(start, size)], weight_sem.at[number]
        )
        copy.start()
        weight_copies.append(copy)

    barrier = pltpu.get_barrier_semaphore()
    for partner in (first_up, first_down, second_up, second_down, pair):
        pl.semaphore_signal(barrier, inc=1, device_id={"vocab": partner}, device_id_type=MESH)

    order = jnp.broadcast_to(order_ref[...].astype(jnp.float32), (LANES, tokens))
    order = jnp.transpose(order)
    lanes = lax.broadcasted_iota(jnp.int32, (tokens, LANES), 1).astype(jnp.float32)
    for start in range(0, tokens, LANES):
        perm[:, pl.ds(start, LANES)] = jnp.where(order == lanes + start, 1.0, 0.0).astype(jnp.bfloat16)
    places = pick_ref[...] - me * width
    places = jnp.concatenate([places, places], axis=1)
    low[...] = places & (LANES - 1)
    high[...] = places >> 7

    own_copy.wait()
    pl.semaphore_wait(barrier, 5)

    started = []

    def push(src, dst, recv, to):
        copy = pltpu.make_async_remote_copy(
            src_ref=src, dst_ref=dst, send_sem=send_sem.at[len(started)], recv_sem=recv,
            device_id={"vocab": to}, device_id_type=MESH,
        )
        copy.start()
        started.append(copy)

    def arrived(rel, half=None):
        ref = block(rel, half)
        pltpu.make_async_remote_copy(
            src_ref=ref, dst_ref=ref, send_sem=send_sem.at[0], recv_sem=recv_sem.at[RECV[rel, half]],
            device_id={"vocab": pair}, device_id_type=MESH,
        ).wait_recv()

    def across(rel, to_rel, to, half=None):
        push(block(rel, half), block(to_rel, half), recv_sem.at[RECV[to_rel, half]], to)

    def to_pair(rel):
        push(block(rel), block(rel, other=1), pair_sem.at[PLACE[rel][0]], pair)

    def along_second(rel):
        across(rel, (rel[0], 3), second_up)
        across(rel, (rel[0], 1), second_down)

    def service(rel):
        if rel in HALVED:
            arrived(rel, 0)
            arrived(rel, 1)
        else:
            arrived(rel)
        if rel == (3, 0):
            across(rel, (2, 0), first_up, 0)
        if rel == (1, 0):
            across(rel, (2, 0), first_down, 1)
        if rel[1] == 0:
            along_second(rel)
        if rel[1] == 3:
            across(rel, (rel[0], 2), second_up, 0)
        if rel[1] == 1:
            across(rel, (rel[0], 2), second_down, 1)
        to_pair(rel)

    def pair_arrived(chunk):
        ref = hidden.at[chunk, pl.ds(BLOCKS * rows, BLOCKS * rows), :]
        pltpu.make_async_remote_copy(
            src_ref=ref, dst_ref=ref, send_sem=send_sem.at[0], recv_sem=pair_sem.at[chunk],
            device_id={"vocab": pair}, device_id_type=MESH,
        ).wait_recv()

    across((0, 0), (3, 0), first_up)
    across((0, 0), (1, 0), first_down)
    along_second((0, 0))
    to_pair((0, 0))
    for rel in ((3, 0), (1, 0), (0, 1), (0, 3)):
        service(rel)

    services = {
        (0, 1): ((2, 0),), (0, 3): ((3, 3), (3, 1)),
        (1, 1): ((1, 1), (1, 3)), (1, 3): ((2, 1), (2, 3)),
        (2, 1): ((0, 2), (3, 2)), (2, 3): ((1, 2), (2, 2)),
    }

    def positions(chunk):
        spots = [None] * (2 * BLOCKS)
        for rel, (number, slot) in PLACE.items():
            if number == chunk:
                spots[slot] = at(*rel, core)
                spots[slot + BLOCKS] = at(*rel, 1 - core)
        return [pl.multiple_of(spot * rows, rows) for spot in spots]

    def digest(chunk, number, spots):
        start, size = tiles[number]
        first = start // LANES
        values = [logits[:, pl.ds(start + LANES * k, LANES)] for k in range(size // LANES)]
        best = functools.reduce(jnp.maximum, values)
        if number == 0:
            total = jnp.zeros_like(best)
            chosen = jnp.zeros_like(best)
        else:
            old = top[...]
            best = jnp.maximum(best, old)
            total = mass[...] * jnp.exp(old - best)
            chosen = found[...]
        lane = jnp.concatenate([low[pl.ds(spot, rows), :] for spot in spots], axis=0)
        tile = jnp.concatenate([high[pl.ds(spot, rows), :] for spot in spots], axis=0)
        for k, value in enumerate(values):
            total = total + jnp.exp(value - best)
            taken = jnp.take_along_axis(value, lane, axis=1, mode="promise_in_bounds")
            chosen = jnp.where(tile == first + k, taken, chosen)
        top[...] = best
        mass[...] = total
        found[...] = chosen

    for chunk in range(4):
        pair_arrived(chunk)
        spots = positions(chunk)
        for number, (start, size) in enumerate(tiles):
            if chunk == 0:
                weight_copies[number].wait()
            logits[:, pl.ds(start, size)] = jnp.dot(
                hidden[chunk], weight[:, pl.ds(start, size)], preferred_element_type=jnp.float32
            )
            if number > 0:
                digest(chunk, number - 1, spots)
            for rel in services.get((chunk, number), ()):
                service(rel)
        digest(chunk, len(tiles) - 1, spots)
        peak = jnp.max(top[...], axis=1, keepdims=True)
        lse = peak + jnp.log(jnp.sum(mass[...] * jnp.exp(top[...] - peak), axis=1, keepdims=True))
        lane = lax.broadcasted_iota(jnp.int32, (chunk_rows, LANES), 1)
        rest = jnp.where(lane < picks, found[...], lse)
        parts = []
        for _ in range(3):
            part = rest.astype(jnp.bfloat16)
            rest = rest - part.astype(jnp.float32)
            parts.append(part)
        parts = jnp.concatenate(parts, axis=1)
        for k, spot in enumerate(spots):
            pieces[pl.ds(spot, rows), :] = parts[k * rows : (k + 1) * rows]

    sorted_parts = jnp.dot(perm[...], pieces[...], preferred_element_type=jnp.float32)
    outbox[...] = (sorted_parts[:, :LANES] + sorted_parts[:, LANES : 2 * LANES]) + sorted_parts[:, 2 * LANES :]

    for step in range(1, SHARDS):
        owner = (me + step) % SHARDS
        pltpu.make_async_remote_copy(
            src_ref=outbox.at[pl.ds(pl.multiple_of(owner * rows, rows), rows), :], dst_ref=inbox.at[step - 1],
            send_sem=out_sem, recv_sem=in_sem, device_id={"vocab": owner}, device_id_type=MESH,
        ).start()
    for copy in started:
        copy.wait_send()
    everything = pltpu.make_async_remote_copy(
        src_ref=inbox, dst_ref=inbox, send_sem=out_sem, recv_sem=in_sem,
        device_id={"vocab": pair}, device_id_type=MESH,
    )
    everything.wait_recv()

    mine = outbox[pl.ds(pl.multiple_of(me * rows, rows), rows), :]
    peak = jnp.maximum(jnp.max(inbox[...], axis=0), mine)
    total = jnp.sum(jnp.exp(inbox[...] - peak[None]), axis=0) + jnp.exp(mine - peak)
    total = (peak + jnp.log(total))[:, picks : picks + 1]
    summed = jnp.sum(inbox[...], axis=0) + mine
    logp_ref[...] = summed[:, :picks] - total
    diagonal = lax.broadcasted_iota(jnp.int32, (rows, rows), 0) == lax.broadcasted_iota(jnp.int32, (rows, rows), 1)
    total_ref[...] = jnp.sum(jnp.where(diagonal, total, 0.0), axis=0, keepdims=True)
    everything.wait_send()


def local(hidden_states, head_weight, pick_index, owner_order):
    rows, depth = hidden_states.shape
    width = head_weight.shape[1]
    tokens, picks = pick_index.shape
    chunk_rows = 2 * BLOCKS * rows
    tile_count = -(-width // TILE)
    logp, total = pl.pallas_call(
        kernel,
        out_shape=(
            jax.ShapeDtypeStruct((rows, picks), jnp.float32),
            jax.ShapeDtypeStruct((1, rows), jnp.float32),
        ),
        in_specs=[
            pl.BlockSpec(memory_space=pl.ANY),
            pl.BlockSpec(memory_space=pl.ANY),
            pl.BlockSpec(memory_space=pltpu.VMEM),
            pl.BlockSpec(memory_space=pltpu.VMEM),
        ],
        out_specs=(pl.BlockSpec(memory_space=pltpu.VMEM), pl.BlockSpec(memory_space=pltpu.VMEM)),
        scratch_shapes=[
            pltpu.VMEM((4, chunk_rows, depth), jnp.bfloat16),
            pltpu.VMEM((depth, width), jnp.bfloat16),
            pltpu.VMEM((chunk_rows, width), jnp.float32),
            pltpu.VMEM((chunk_rows, LANES), jnp.float32),
            pltpu.VMEM((chunk_rows, LANES), jnp.float32),
            pltpu.VMEM((chunk_rows, LANES), jnp.float32),
            pltpu.VMEM((tokens, LANES), jnp.int32),
            pltpu.VMEM((tokens, LANES), jnp.int32),
            pltpu.VMEM((tokens, 3 * LANES), jnp.bfloat16),
            pltpu.VMEM((tokens, tokens), jnp.bfloat16),
            pltpu.VMEM((tokens, LANES), jnp.float32),
            pltpu.VMEM((SHARDS - 1, rows, LANES), jnp.float32),
            pltpu.SemaphoreType.DMA,
            pltpu.SemaphoreType.DMA((tile_count,)),
            pltpu.SemaphoreType.DMA((SENDS,)),
            pltpu.SemaphoreType.DMA((len(ARRIVALS),)),
            pltpu.SemaphoreType.DMA((4,)),
            pltpu.SemaphoreType.DMA,
            pltpu.SemaphoreType.DMA,
        ],
        compiler_params=pltpu.CompilerParams(
            collective_id=0, has_side_effects=True, vmem_limit_bytes=62 * 1024 * 1024
        ),
    )(hidden_states, head_weight, pick_index, owner_order.reshape(1, tokens))
    return logp, total.reshape(rows)


def solution(mesh):
    in_specs = (P(("group", "vocab"), None), P(None, "vocab"), P("group", None), P("group"))
    out_specs = (P(("group", "vocab"), None), P(("group", "vocab")))
    return jax.shard_map(local, mesh=mesh, in_specs=in_specs, out_specs=out_specs, check_vma=False)
```

```python
import functools

import jax
import jax.numpy as jnp
from jax import lax
from jax.experimental import pallas as pl
from jax.experimental.pallas import tpu as pltpu
from jax.sharding import PartitionSpec as P

MESH = pl.DeviceIdType.MESH
SIDE = 4
SHARDS = 2 * SIDE * SIDE
LANES = 128
TILE = 512
BLOCKS = 4
PLACE = {
    (0, 0): (0, 0), (3, 0): (0, 1), (1, 0): (0, 2), (0, 1): (0, 3),
    (0, 3): (1, 0), (2, 0): (1, 1), (0, 2): (1, 2), (3, 1): (1, 3),
    (3, 3): (2, 0), (1, 1): (2, 1), (1, 3): (2, 2), (2, 1): (2, 3),
    (2, 3): (3, 0), (2, 2): (3, 1), (3, 2): (3, 2), (1, 2): (3, 3),
}
HALVED = ((3, 2), (1, 2))
WHOLE = tuple(rel for rel in PLACE if rel not in HALVED and rel != (0, 0))
ARRIVALS = [(rel, None) for rel in WHOLE] + [(rel, half) for rel in HALVED for half in (0, 1)]
RECV = {key: number for number, key in enumerate(ARRIVALS)}
OTHERS = sorted(
    ((dx, dz, dc) for dx in range(SIDE) for dz in range(SIDE) for dc in range(2) if dx or dz or dc),
    key=lambda step: -min(step[0], SIDE - step[0]) - min(step[1], SIDE - step[1]),
)
SENDS = 40


def flat(x, z, core):
    return ((x % SIDE) * SIDE + z % SIDE) * 2 + core


def kernel(
    x_ref, w_ref, pick_ref, order_ref, logp_ref, total_ref,
    hidden, weight, logits, top, mass, found, chosen_ref, low, high, pieces, perm,
    outbox, inbox, sums_out, sums_in,
    own_sem, pick_sem, weight_sem, send_sem, recv_sem, pair_sem, out_sem, in_sem, sums_out_sem, sums_in_sem,
):
    rows, depth = x_ref.shape
    width = w_ref.shape[1]
    picks, tokens = pick_ref.shape
    half_depth = depth // 2
    chunk_rows = 2 * BLOCKS * rows
    tiles = [(start, min(TILE, width - start)) for start in range(0, width, TILE)]

    me = lax.axis_index("vocab")
    core = me % 2
    x = me // 2 // SIDE
    z = me // 2 % SIDE
    pair = me + 1 - 2 * core

    def at(da, db, kind):
        return (1 - kind) * flat(x + da, z + db, kind) + kind * flat(x + db, z + da, kind)

    first_up, first_down = at(1, 0, core), at(3, 0, core)
    second_up, second_down = at(0, 1, core), at(0, 3, core)
    first_far, second_far = at(2, 0, core), at(0, 2, core)

    def block(rel, half=None, other=0):
        chunk, slot = PLACE[rel]
        row = (slot + BLOCKS * other) * rows
        if half is None:
            return hidden.at[chunk, pl.ds(row, rows), :]
        return hidden.at[chunk, pl.ds(row, rows), pl.ds(half * half_depth, half_depth)]

    own_copy = pltpu.make_async_copy(x_ref, block((0, 0)), own_sem)
    own_copy.start()
    pick_copy = pltpu.make_async_copy(pick_ref, chosen_ref, pick_sem)
    pick_copy.start()
    weight_copies = []
    for number, (start, size) in enumerate(tiles):
        copy = pltpu.make_async_copy(
            w_ref.at[:, pl.ds(start, size)], weight.at[:, pl.ds(start, size)], weight_sem.at[number]
        )
        copy.start()
        weight_copies.append(copy)

    barrier = pltpu.get_barrier_semaphore()
    for partner in (first_up, first_down, second_up, second_down, first_far, second_far, pair):
        pl.semaphore_signal(barrier, inc=1, device_id={"vocab": partner}, device_id_type=MESH)

    own_copy.wait()
    pl.semaphore_wait(barrier, 7)

    started = []

    def push(src, dst, recv, to):
        copy = pltpu.make_async_remote_copy(
            src_ref=src, dst_ref=dst, send_sem=send_sem.at[len(started)], recv_sem=recv,
            device_id={"vocab": to}, device_id_type=MESH,
        )
        copy.start()
        started.append(copy)

    def arrived(rel, half=None):
        ref = block(rel, half)
        pltpu.make_async_remote_copy(
            src_ref=ref, dst_ref=ref, send_sem=send_sem.at[0], recv_sem=recv_sem.at[RECV[rel, half]],
            device_id={"vocab": pair}, device_id_type=MESH,
        ).wait_recv()

    def across(rel, to_rel, to, half=None):
        push(block(rel, half), block(to_rel, half), recv_sem.at[RECV[to_rel, half]], to)

    def to_pair(rel):
        push(block(rel), block(rel, other=1), pair_sem.at[PLACE[rel][0]], pair)

    def along_second(rel):
        across(rel, (rel[0], 3), second_up)
        across(rel, (rel[0], 1), second_down)

    def service(rel):
        if rel in HALVED:
            arrived(rel, 0)
            arrived(rel, 1)
        else:
            arrived(rel)
        if rel[1] == 0:
            along_second(rel)
        if rel == (2, 0):
            across(rel, (2, 2), second_far)
        if rel[0] in (1, 3) and rel[1] == 3:
            across(rel, (rel[0], 2), second_up, 0)
        if rel[0] in (1, 3) and rel[1] == 1:
            across(rel, (rel[0], 2), second_down, 1)
        to_pair(rel)

    def pair_arrived(chunk):
        ref = hidden.at[chunk, pl.ds(BLOCKS * rows, BLOCKS * rows), :]
        pltpu.make_async_remote_copy(
            src_ref=ref, dst_ref=ref, send_sem=send_sem.at[0], recv_sem=pair_sem.at[chunk],
            device_id={"vocab": pair}, device_id_type=MESH,
        ).wait_recv()

    across((0, 0), (3, 0), first_up)
    across((0, 0), (1, 0), first_down)
    along_second((0, 0))
    to_pair((0, 0))
    across((0, 0), (2, 0), first_far)
    across((0, 0), (0, 2), second_far)

    order = jnp.broadcast_to(order_ref[...].astype(jnp.float32), (LANES, tokens))
    order = jnp.transpose(order).reshape(SHARDS, 2, rows // 2, LANES)
    order = jnp.concatenate([order[:, 0].reshape(-1, LANES), order[:, 1].reshape(-1, LANES)], axis=0)
    lanes = lax.broadcasted_iota(jnp.int32, (tokens, LANES), 1).astype(jnp.float32)
    for start in range(0, tokens, LANES):
        perm[:, pl.ds(start, LANES)] = jnp.where(order == lanes + start, 1.0, 0.0).astype(jnp.bfloat16)
    pick_copy.wait()
    for start in range(0, tokens, LANES):
        places = chosen_ref[:, pl.ds(start, LANES)] - me * width
        places = jnp.transpose(jnp.concatenate([places, places], axis=0))
        low[pl.ds(start, LANES), :] = places & (LANES - 1)
        high[pl.ds(start, LANES), :] = places >> 7

    for rel in ((3, 0), (1, 0), (0, 1), (0, 3)):
        service(rel)

    services = {
        (0, 2): ((2, 0), (0, 2)), (0, 4): ((3, 1), (3, 3)),
        (1, 1): ((1, 1), (1, 3)), (1, 3): ((2, 1), (2, 3)),
        (2, 2): ((2, 2),), (2, 4): ((3, 2), (1, 2)),
    }

    def positions(chunk):
        spots = [None] * (2 * BLOCKS)
        for rel, (number, slot) in PLACE.items():
            if number == chunk:
                spots[slot] = at(*rel, core)
                spots[slot + BLOCKS] = at(*rel, 1 - core)
        return [pl.multiple_of(spot * rows, rows) for spot in spots]

    def digest(chunk, number, spots):
        start, size = tiles[number]
        first = start // LANES
        values = [logits[:, pl.ds(start + LANES * k, LANES)] for k in range(size // LANES)]
        best = functools.reduce(jnp.maximum, values)
        if number == 0:
            total = jnp.zeros_like(best)
            chosen = jnp.zeros_like(best)
        else:
            old = top[...]
            best = jnp.maximum(best, old)
            total = mass[...] * jnp.exp(old - best)
            chosen = found[...]
        lane = jnp.concatenate([low[pl.ds(spot, rows), :] for spot in spots], axis=0)
        tile = jnp.concatenate([high[pl.ds(spot, rows), :] for spot in spots], axis=0)
        for k, value in enumerate(values):
            total = total + jnp.exp(value - best)
            taken = jnp.take_along_axis(value, lane, axis=1, mode="promise_in_bounds")
            chosen = jnp.where(tile == first + k, taken, chosen)
        top[...] = best
        mass[...] = total
        found[...] = chosen

    for chunk in range(4):
        pair_arrived(chunk)
        spots = positions(chunk)
        for number, (start, size) in enumerate(tiles):
            if chunk == 0:
                weight_copies[number].wait()
            logits[:, pl.ds(start, size)] = jnp.dot(
                hidden[chunk], weight[:, pl.ds(start, size)], preferred_element_type=jnp.float32
            )
            if number > 0:
                digest(chunk, number - 1, spots)
            for rel in services.get((chunk, number), ()):
                service(rel)
        digest(chunk, len(tiles) - 1, spots)
        peak = jnp.max(top[...], axis=1, keepdims=True)
        lse = peak + jnp.log(jnp.sum(mass[...] * jnp.exp(top[...] - peak), axis=1, keepdims=True))
        lane = lax.broadcasted_iota(jnp.int32, (chunk_rows, LANES), 1)
        rest = jnp.where(lane < picks, found[...], lse)
        parts = []
        for _ in range(3):
            part = rest.astype(jnp.bfloat16)
            rest = rest - part.astype(jnp.float32)
            parts.append(part)
        parts = jnp.concatenate(parts, axis=1)
        for k, spot in enumerate(spots):
            pieces[pl.ds(spot, rows), :] = parts[k * rows : (k + 1) * rows]

    parts = jnp.dot(perm[...], pieces[...], preferred_element_type=jnp.float32)
    ordered = (parts[:, :LANES] + parts[:, LANES : 2 * LANES]) + parts[:, 2 * LANES :]
    upper, lower = ordered[: tokens // 2], ordered[tokens // 2 :]
    lane = lax.broadcasted_iota(jnp.int32, upper.shape, 1)
    outbox[...] = jnp.where(lane < picks, upper, pltpu.roll(lower, picks, 1)).reshape(outbox.shape)
    step = lax.broadcasted_iota(jnp.int32, upper.shape, 0) % (rows // 2)
    sums = jnp.where(lane == picks + step, upper, 0.0) + jnp.where(lane == picks + rows // 2 + step, lower, 0.0)
    for shard in range(SHARDS):
        part = sums[shard * (rows // 2) : (shard + 1) * (rows // 2)]
        sums_out[shard] = jnp.sum(part, axis=0, keepdims=True)

    for number, (dx, dz, dc) in enumerate(OTHERS):
        owner = flat(x + dx, z + dz, (core + dc) % 2)
        for source, target, sends, receives in (
            (outbox, inbox, out_sem, in_sem), (sums_out, sums_in, sums_out_sem, sums_in_sem)
        ):
            pltpu.make_async_remote_copy(
                src_ref=source.at[owner], dst_ref=target.at[number], send_sem=sends, recv_sem=receives,
                device_id={"vocab": owner}, device_id_type=MESH,
            ).start()
    for copy in started:
        copy.wait_send()

    def exchanged(target, sends, receives):
        return pltpu.make_async_remote_copy(
            src_ref=target, dst_ref=target, send_sem=sends, recv_sem=receives,
            device_id={"vocab": pair}, device_id_type=MESH,
        )

    picks_moved = exchanged(inbox, out_sem, in_sem)
    sums_moved = exchanged(sums_in, sums_out_sem, sums_in_sem)
    sums_moved.wait_recv()
    own_sum = sums_out[me]
    peak = jnp.maximum(jnp.max(sums_in[...], axis=0), own_sum)
    total = jnp.sum(jnp.exp(sums_in[...] - peak[None]), axis=0) + jnp.exp(own_sum - peak)
    total = peak + jnp.log(total)
    total_ref[...] = total[:, picks : picks + rows]
    lane = lax.broadcasted_iota(jnp.int32, (rows // 2, LANES), 1)
    step = lax.broadcasted_iota(jnp.int32, (rows // 2, LANES), 0)
    spread = jnp.broadcast_to(total, (rows // 2, LANES))
    first = jnp.sum(jnp.where(lane == picks + step, spread, 0.0), axis=1, keepdims=True)
    second = jnp.sum(jnp.where(lane == picks + rows // 2 + step, spread, 0.0), axis=1, keepdims=True)
    picks_moved.wait_recv()
    summed = jnp.sum(inbox[...], axis=0) + outbox[me] - jnp.where(lane < picks, first, second)
    logp_ref[pl.ds(0, rows // 2), :] = summed[:, :picks]
    logp_ref[pl.ds(rows // 2, rows // 2), :] = pltpu.roll(summed, picks, 1)[:, :picks]
    sums_moved.wait_send()
    picks_moved.wait_send()


def local(hidden_states, head_weight, pick_index, owner_order):
    rows, depth = hidden_states.shape
    width = head_weight.shape[1]
    tokens, picks = pick_index.shape
    chunk_rows = 2 * BLOCKS * rows
    tile_count = -(-width // TILE)
    logp, total = pl.pallas_call(
        kernel,
        out_shape=(
            jax.ShapeDtypeStruct((rows, picks), jnp.float32),
            jax.ShapeDtypeStruct((1, rows), jnp.float32),
        ),
        in_specs=[
            pl.BlockSpec(memory_space=pl.ANY),
            pl.BlockSpec(memory_space=pl.ANY),
            pl.BlockSpec(memory_space=pl.ANY),
            pl.BlockSpec(memory_space=pltpu.VMEM),
        ],
        out_specs=(pl.BlockSpec(memory_space=pltpu.VMEM), pl.BlockSpec(memory_space=pltpu.VMEM)),
        scratch_shapes=[
            pltpu.VMEM((4, chunk_rows, depth), jnp.bfloat16),
            pltpu.VMEM((depth, width), jnp.bfloat16),
            pltpu.VMEM((chunk_rows, width), jnp.float32),
            pltpu.VMEM((chunk_rows, LANES), jnp.float32),
            pltpu.VMEM((chunk_rows, LANES), jnp.float32),
            pltpu.VMEM((chunk_rows, LANES), jnp.float32),
            pltpu.VMEM((picks, tokens), jnp.int32),
            pltpu.VMEM((tokens, LANES), jnp.int32),
            pltpu.VMEM((tokens, LANES), jnp.int32),
            pltpu.VMEM((tokens, 3 * LANES), jnp.bfloat16),
            pltpu.VMEM((tokens, tokens), jnp.bfloat16),
            pltpu.VMEM((SHARDS, rows // 2, LANES), jnp.float32),
            pltpu.VMEM((SHARDS - 1, rows // 2, LANES), jnp.float32),
            pltpu.VMEM((SHARDS, 1, LANES), jnp.float32),
            pltpu.VMEM((SHARDS - 1, 1, LANES), jnp.float32),
            pltpu.SemaphoreType.DMA,
            pltpu.SemaphoreType.DMA,
            pltpu.SemaphoreType.DMA((tile_count,)),
            pltpu.SemaphoreType.DMA((SENDS,)),
            pltpu.SemaphoreType.DMA((len(ARRIVALS),)),
            pltpu.SemaphoreType.DMA((4,)),
            pltpu.SemaphoreType.DMA,
            pltpu.SemaphoreType.DMA,
            pltpu.SemaphoreType.DMA,
            pltpu.SemaphoreType.DMA,
        ],
        compiler_params=pltpu.CompilerParams(
            collective_id=0, has_side_effects=True, vmem_limit_bytes=62 * 1024 * 1024
        ),
    )(hidden_states, head_weight, pick_index.T, owner_order.reshape(1, tokens))
    return logp, total.reshape(rows)


def solution(mesh):
    in_specs = (P(("group", "vocab"), None), P(None, "vocab"), P("group", None), P("group"))
    out_specs = (P(("group", "vocab"), None), P(("group", "vocab")))
    return jax.shard_map(local, mesh=mesh, in_specs=in_specs, out_specs=out_specs, check_vma=False)
```

```python
import functools

import jax
import jax.numpy as jnp
from jax import lax
from jax.experimental import pallas as pl
from jax.experimental.pallas import tpu as pltpu
from jax.sharding import PartitionSpec as P

MESH = pl.DeviceIdType.MESH
SIDE = 4
SHARDS = 2 * SIDE * SIDE
LANES = 128
TILE = 512
BLOCKS = 4
PLACE = {
    (0, 0): (0, 0), (3, 0): (0, 1), (1, 0): (0, 2), (0, 1): (0, 3),
    (0, 3): (1, 0), (2, 0): (1, 1), (0, 2): (1, 2), (3, 1): (1, 3),
    (3, 3): (2, 0), (1, 1): (2, 1), (1, 3): (2, 2), (2, 1): (2, 3),
    (2, 3): (3, 0), (2, 2): (3, 1), (3, 2): (3, 2), (1, 2): (3, 3),
}
PIECES = {rel: 1 for rel in PLACE if rel != (0, 0)}
PIECES.update({rel: 2 for rel in ((3, 0), (1, 0), (3, 1), (3, 3), (1, 1), (1, 3), (2, 0), (0, 2), (3, 2), (1, 2), (2, 2))})
RECV = {}
for rel, count in PIECES.items():
    for piece in range(count):
        RECV[rel, piece] = len(RECV)
OTHERS = sorted(
    ((dx, dz, dc) for dx in range(SIDE) for dz in range(SIDE) for dc in range(2) if dx or dz or dc),
    key=lambda step: -min(step[0], SIDE - step[0]) - min(step[1], SIDE - step[1]),
)
SENDS = 80


def flat(x, z, core):
    return ((x % SIDE) * SIDE + z % SIDE) * 2 + core


def kernel(
    x_ref, w_ref, pick_ref, order_ref, logp_ref, total_ref,
    hidden, weight, logits, top, mass, found, chosen_ref, order_row, low, high, pieces, perm,
    outbox, inbox, sums_out, sums_in,
    own_sem, pick_sem, order_sem, weight_sem, send_sem, recv_sem, pair_sem, out_sem, in_sem, sums_out_sem, sums_in_sem,
):
    rows, depth = x_ref.shape
    width = w_ref.shape[1]
    picks, tokens = pick_ref.shape
    chunk_rows = 2 * BLOCKS * rows
    tiles = [(start, min(TILE, width - start)) for start in range(0, width, TILE)]

    me = lax.axis_index("vocab")
    core = me % 2
    x = me // 2 // SIDE
    z = me // 2 % SIDE
    pair = me + 1 - 2 * core

    def at(da, db, kind):
        return (1 - kind) * flat(x + da, z + db, kind) + kind * flat(x + db, z + da, kind)

    first_up, first_down = at(1, 0, core), at(3, 0, core)
    second_up, second_down = at(0, 1, core), at(0, 3, core)

    def block(rel, piece=0, pieces=1, other=0):
        chunk, slot = PLACE[rel]
        size = depth // pieces
        return hidden.at[chunk, pl.ds((slot + BLOCKS * other) * rows, rows), pl.ds(piece * size, size)]

    own_copy = pltpu.make_async_copy(x_ref, block((0, 0)), own_sem)
    own_copy.start()
    pick_copy = pltpu.make_async_copy(pick_ref, chosen_ref, pick_sem)
    pick_copy.start()
    order_copy = pltpu.make_async_copy(order_ref, order_row, order_sem)
    order_copy.start()
    weight_copies = []
    for number, (start, size) in enumerate(tiles):
        copy = pltpu.make_async_copy(
            w_ref.at[:, pl.ds(start, size)], weight.at[:, pl.ds(start, size)], weight_sem.at[number]
        )
        copy.start(priority=1)
        weight_copies.append(copy)

    barrier = pltpu.get_barrier_semaphore()
    for partner in (first_up, first_down, second_up, second_down, pair):
        pl.semaphore_signal(barrier, inc=1, device_id={"vocab": partner}, device_id_type=MESH)

    own_copy.wait()
    pl.semaphore_wait(barrier, 5)

    started = []

    def push(src, dst, recv, to):
        copy = pltpu.make_async_remote_copy(
            src_ref=src, dst_ref=dst, send_sem=send_sem.at[len(started)], recv_sem=recv,
            device_id={"vocab": to}, device_id_type=MESH,
        )
        copy.start()
        started.append(copy)

    def wait_for(ref, sem):
        pltpu.make_async_remote_copy(
            src_ref=ref, dst_ref=ref, send_sem=send_sem.at[0], recv_sem=sem,
            device_id={"vocab": pair}, device_id_type=MESH,
        ).wait_recv()

    def arrived(rel, *pieces):
        for piece in pieces or range(PIECES[rel]):
            wait_for(block(rel, piece, PIECES[rel]), recv_sem.at[RECV[rel, piece]])

    def across(rel, to_rel, to, piece=0):
        count = PIECES[to_rel]
        push(block(rel, piece, count), block(to_rel, piece, count), recv_sem.at[RECV[to_rel, piece]], to)

    def along_second(rel, piece=0):
        across(rel, (rel[0], 3), second_up, piece)
        across(rel, (rel[0], 1), second_down, piece)

    def to_pair(rel):
        push(block(rel), block(rel, other=1), pair_sem.at[PLACE[rel][0]], pair)

    def service(rel):
        arrived(rel)
        if rel == (2, 0):
            along_second(rel)
        elif rel[1] == 3:
            across(rel, (rel[0], 2), second_up, 0)
        elif rel[1] == 1:
            across(rel, (rel[0], 2), second_down, 1)
        to_pair(rel)

    def pair_arrived(chunk):
        wait_for(hidden.at[chunk, pl.ds(BLOCKS * rows, BLOCKS * rows), :], pair_sem.at[chunk])

    across((0, 0), (3, 0), first_up, 0)
    across((0, 0), (1, 0), first_down, 1)
    along_second((0, 0))
    across((0, 0), (3, 0), first_up, 1)
    across((0, 0), (1, 0), first_down, 0)
    to_pair((0, 0))

    order_copy.wait()
    order = jnp.broadcast_to(order_row[...].astype(jnp.float32), (LANES, tokens))
    order = jnp.transpose(order).reshape(SHARDS, 2, rows // 2, LANES)
    order = jnp.concatenate([order[:, 0].reshape(-1, LANES), order[:, 1].reshape(-1, LANES)], axis=0)
    lanes = lax.broadcasted_iota(jnp.int32, (tokens, LANES), 1).astype(jnp.float32)
    for start in range(0, tokens, LANES):
        perm[:, pl.ds(start, LANES)] = jnp.where(order == lanes + start, 1.0, 0.0).astype(jnp.bfloat16)
    pick_copy.wait()
    for start in range(0, tokens, LANES):
        places = chosen_ref[:, pl.ds(start, LANES)] - me * width
        places = jnp.transpose(jnp.concatenate([places, places], axis=0))
        low[pl.ds(start, LANES), :] = places & (LANES - 1)
        high[pl.ds(start, LANES), :] = places >> 7

    for turn in (0, 1):
        for rel, half, on in (((3, 0), turn, first_up), ((1, 0), 1 - turn, first_down)):
            arrived(rel, half)
            if turn == 0:
                across(rel, (2, 0), on, half)
            along_second(rel, half)
            if turn == 1:
                to_pair(rel)
    service((0, 1))
    service((0, 3))

    services = {
        (0, 2): ((2, 0),), (0, 4): ((0, 2), (3, 3), (3, 1), (1, 1), (1, 3)),
        (1, 1): ((2, 1), (2, 3)), (2, 2): ((2, 2), (3, 2), (1, 2)),
    }

    def positions(chunk):
        spots = [None] * (2 * BLOCKS)
        for rel, (number, slot) in PLACE.items():
            if number == chunk:
                spots[slot] = at(*rel, core)
                spots[slot + BLOCKS] = at(*rel, 1 - core)
        return [pl.multiple_of(spot * rows, rows) for spot in spots]

    def digest(chunk, number, spots):
        start, size = tiles[number]
        first = start // LANES
        values = [logits[:, pl.ds(start + LANES * k, LANES)] for k in range(size // LANES)]
        best = functools.reduce(jnp.maximum, values)
        if number == 0:
            total = jnp.zeros_like(best)
            chosen = jnp.zeros_like(best)
        else:
            old = top[...]
            best = jnp.maximum(best, old)
            total = mass[...] * jnp.exp(old - best)
            chosen = found[...]
        lane = jnp.concatenate([low[pl.ds(spot, rows), :] for spot in spots], axis=0)
        tile = jnp.concatenate([high[pl.ds(spot, rows), :] for spot in spots], axis=0)
        for k, value in enumerate(values):
            total = total + jnp.exp(value - best)
            taken = jnp.take_along_axis(value, lane, axis=1, mode="promise_in_bounds")
            chosen = jnp.where(tile == first + k, taken, chosen)
        top[...] = best
        mass[...] = total
        found[...] = chosen

    def finish(chunk, spots):
        digest(chunk, len(tiles) - 1, spots)
        peak = jnp.max(top[...], axis=1, keepdims=True)
        lse = peak + jnp.log(jnp.sum(mass[...] * jnp.exp(top[...] - peak), axis=1, keepdims=True))
        lane = lax.broadcasted_iota(jnp.int32, (chunk_rows, LANES), 1)
        rest = jnp.where(lane < picks, found[...], lse)
        parts = []
        for _ in range(2):
            part = rest.astype(jnp.bfloat16)
            rest = rest - part.astype(jnp.float32)
            parts.append(part)
        parts = jnp.concatenate(parts, axis=1)
        for k, spot in enumerate(spots):
            pieces[pl.ds(spot, rows), :] = parts[k * rows : (k + 1) * rows]

    for chunk in range(4):
        pair_arrived(chunk)
        if chunk == 0:
            for copy in weight_copies:
                copy.wait()
        for number, (start, size) in enumerate(tiles):
            logits[:, pl.ds(start, size)] = jnp.dot(
                hidden[chunk], weight[:, pl.ds(start, size)], preferred_element_type=jnp.float32
            )
            if number > 0:
                digest(chunk, number - 1, positions(chunk))
            elif chunk > 0:
                finish(chunk - 1, positions(chunk - 1))
            for rel in services.get((chunk, number), ()):
                service(rel)
    finish(3, positions(3))

    parts = jnp.dot(perm[...], pieces[...], preferred_element_type=jnp.float32)
    ordered = parts[:, :LANES] + parts[:, LANES:]
    upper, lower = ordered[: tokens // 2], ordered[tokens // 2 :]
    lane = lax.broadcasted_iota(jnp.int32, upper.shape, 1)
    outbox[...] = jnp.where(lane < picks, upper, pltpu.roll(lower, picks, 1)).reshape(outbox.shape)
    step = lax.broadcasted_iota(jnp.int32, upper.shape, 0) % (rows // 2)
    sums = jnp.where(lane == picks + step, upper, 0.0) + jnp.where(lane == picks + rows // 2 + step, lower, 0.0)
    for shard in range(SHARDS):
        part = sums[shard * (rows // 2) : (shard + 1) * (rows // 2)]
        sums_out[shard] = jnp.sum(part, axis=0, keepdims=True)

    for number, (dx, dz, dc) in enumerate(OTHERS):
        owner = flat(x + dx, z + dz, (core + dc) % 2)
        for source, target, sends, receives in (
            (outbox, inbox, out_sem, in_sem), (sums_out, sums_in, sums_out_sem, sums_in_sem)
        ):
            pltpu.make_async_remote_copy(
                src_ref=source.at[owner], dst_ref=target.at[number], send_sem=sends, recv_sem=receives,
                device_id={"vocab": owner}, device_id_type=MESH,
            ).start()
    for copy in started:
        copy.wait_send()

    def exchanged(target, sends, receives):
        return pltpu.make_async_remote_copy(
            src_ref=target, dst_ref=target, send_sem=sends, recv_sem=receives,
            device_id={"vocab": pair}, device_id_type=MESH,
        )

    picks_moved = exchanged(inbox, out_sem, in_sem)
    sums_moved = exchanged(sums_in, sums_out_sem, sums_in_sem)
    sums_moved.wait_recv()
    own_sum = sums_out[me]
    peak = jnp.maximum(jnp.max(sums_in[...], axis=0), own_sum)
    total = jnp.sum(jnp.exp(sums_in[...] - peak[None]), axis=0) + jnp.exp(own_sum - peak)
    total = peak + jnp.log(total)
    total_ref[...] = total[:, picks : picks + rows]
    lane = lax.broadcasted_iota(jnp.int32, (rows // 2, LANES), 1)
    step = lax.broadcasted_iota(jnp.int32, (rows // 2, LANES), 0)
    spread = jnp.broadcast_to(total, (rows // 2, LANES))
    first = jnp.sum(jnp.where(lane == picks + step, spread, 0.0), axis=1, keepdims=True)
    second = jnp.sum(jnp.where(lane == picks + rows // 2 + step, spread, 0.0), axis=1, keepdims=True)
    picks_moved.wait_recv()
    summed = jnp.sum(inbox[...], axis=0) + outbox[me] - jnp.where(lane < picks, first, second)
    logp_ref[pl.ds(0, rows // 2), :] = summed[:, :picks]
    logp_ref[pl.ds(rows // 2, rows // 2), :] = pltpu.roll(summed, picks, 1)[:, :picks]
    sums_moved.wait_send()
    picks_moved.wait_send()


def local(hidden_states, head_weight, pick_index, owner_order):
    rows, depth = hidden_states.shape
    width = head_weight.shape[1]
    tokens, picks = pick_index.shape
    chunk_rows = 2 * BLOCKS * rows
    tile_count = -(-width // TILE)
    operands = (hidden_states, head_weight, pick_index.T, owner_order.reshape(1, tokens))
    logp, total = pl.pallas_call(
        kernel,
        out_shape=(
            jax.ShapeDtypeStruct((rows, picks), jnp.float32),
            jax.ShapeDtypeStruct((1, rows), jnp.float32),
        ),
        in_specs=[
            pl.BlockSpec(memory_space=pltpu.HBM),
            pl.BlockSpec(memory_space=pltpu.HBM),
            pl.BlockSpec(memory_space=pltpu.HBM),
            pl.BlockSpec(memory_space=pltpu.HBM),
        ],
        out_specs=(pl.BlockSpec(memory_space=pltpu.VMEM), pl.BlockSpec(memory_space=pltpu.VMEM)),
        scratch_shapes=[
            pltpu.VMEM((4, chunk_rows, depth), jnp.bfloat16),
            pltpu.VMEM((depth, width), jnp.bfloat16),
            pltpu.VMEM((chunk_rows, width), jnp.float32),
            pltpu.VMEM((chunk_rows, LANES), jnp.float32),
            pltpu.VMEM((chunk_rows, LANES), jnp.float32),
            pltpu.VMEM((chunk_rows, LANES), jnp.float32),
            pltpu.VMEM((picks, tokens), jnp.int32),
            pltpu.VMEM((1, tokens), jnp.int32),
            pltpu.VMEM((tokens, LANES), jnp.int32),
            pltpu.VMEM((tokens, LANES), jnp.int32),
            pltpu.VMEM((tokens, 2 * LANES), jnp.bfloat16),
            pltpu.VMEM((tokens, tokens), jnp.bfloat16),
            pltpu.VMEM((SHARDS, rows // 2, LANES), jnp.float32),
            pltpu.VMEM((SHARDS - 1, rows // 2, LANES), jnp.float32),
            pltpu.VMEM((SHARDS, 1, LANES), jnp.float32),
            pltpu.VMEM((SHARDS - 1, 1, LANES), jnp.float32),
            pltpu.SemaphoreType.DMA,
            pltpu.SemaphoreType.DMA,
            pltpu.SemaphoreType.DMA,
            pltpu.SemaphoreType.DMA((tile_count,)),
            pltpu.SemaphoreType.DMA((SENDS,)),
            pltpu.SemaphoreType.DMA((len(RECV),)),
            pltpu.SemaphoreType.DMA((4,)),
            pltpu.SemaphoreType.DMA,
            pltpu.SemaphoreType.DMA,
            pltpu.SemaphoreType.DMA,
            pltpu.SemaphoreType.DMA,
        ],
        compiler_params=pltpu.CompilerParams(
            collective_id=0, has_side_effects=True, vmem_limit_bytes=48 * 1024 * 1024
        ),
    )(*(pltpu.with_memory_space_constraint(a, pltpu.HBM) for a in operands))
    return logp, total.reshape(rows)


def solution(mesh):
    in_specs = (P(("group", "vocab"), None), P(None, "vocab"), P("group", None), P("group"))
    out_specs = (P(("group", "vocab"), None), P(("group", "vocab")))
    return jax.shard_map(local, mesh=mesh, in_specs=in_specs, out_specs=out_specs, check_vma=False)
```

```python
import functools

import jax
import jax.numpy as jnp
from jax import lax
from jax.experimental import pallas as pl
from jax.experimental.pallas import tpu as pltpu
from jax.sharding import PartitionSpec as P

MESH = pl.DeviceIdType.MESH
SIDE = 4
SHARDS = 2 * SIDE * SIDE
LANES = 128
TILE = 512
OWN = (
    ((0, 0), (3, 0), (1, 0), (0, 1), (0, 3)),
    ((2, 0), (3, 3), (3, 1), (1, 1)),
    ((1, 3), (2, 1), (2, 3), (0, 2)),
    ((2, 2), (3, 2), (1, 2)),
)
HANDED = (
    ((0, 0), (3, 0), (1, 0)),
    ((0, 1), (0, 3), (2, 0), (3, 3)),
    ((3, 1), (1, 1), (1, 3), (2, 1)),
    ((2, 3), (0, 2), (2, 2), (3, 2), (1, 2)),
)
COUNTS = tuple(len(own) + len(handed) for own, handed in zip(OWN, HANDED))
PLACE = {rel: (chunk, slot) for chunk, rels in enumerate(OWN) for slot, rel in enumerate(rels)}
PLACE_HANDED = {
    rel: (chunk, len(OWN[chunk]) + slot) for chunk, rels in enumerate(HANDED) for slot, rel in enumerate(rels)
}
PIECES = {rel: 1 for rel in PLACE if rel != (0, 0)}
PIECES.update({rel: 2 for rel in ((3, 0), (1, 0), (3, 1), (3, 3), (1, 1), (1, 3), (2, 0), (0, 2), (3, 2), (1, 2), (2, 2))})
RECV = {}
for rel, count in PIECES.items():
    for piece in range(count):
        RECV[rel, piece] = len(RECV)
OTHERS = sorted(
    ((dx, dz, dc) for dx in range(SIDE) for dz in range(SIDE) for dc in range(2) if dx or dz or dc),
    key=lambda step: -min(step[0], SIDE - step[0]) - min(step[1], SIDE - step[1]),
)
SENDS = 80


def flat(x, z, core):
    return ((x % SIDE) * SIDE + z % SIDE) * 2 + core


def kernel(
    x_ref, w_ref, pick_ref, order_ref, logp_ref, total_ref,
    hidden, weight, logits, top, mass, found, chosen_ref, order_row, low, high, pieces, perm,
    outbox, inbox, sums_out, sums_in,
    own_sem, pick_sem, order_sem, weight_sem, send_sem, recv_sem, pair_sem, out_sem, in_sem, sums_out_sem, sums_in_sem,
):
    rows, depth = x_ref.shape
    width = w_ref.shape[1]
    picks, tokens = pick_ref.shape
    tiles = [(start, min(TILE, width - start)) for start in range(0, width, TILE)]

    me = lax.axis_index("vocab")
    core = me % 2
    x = me // 2 // SIDE
    z = me // 2 % SIDE
    pair = me + 1 - 2 * core

    def at(da, db, kind):
        return (1 - kind) * flat(x + da, z + db, kind) + kind * flat(x + db, z + da, kind)

    first_up, first_down = at(1, 0, core), at(3, 0, core)
    second_up, second_down = at(0, 1, core), at(0, 3, core)

    def block(rel, piece=0, pieces=1, other=0):
        chunk, slot = (PLACE_HANDED if other else PLACE)[rel]
        size = depth // pieces
        return hidden.at[chunk, pl.ds(slot * rows, rows), pl.ds(piece * size, size)]

    own_copy = pltpu.make_async_copy(x_ref, block((0, 0)), own_sem)
    own_copy.start()
    pick_copy = pltpu.make_async_copy(pick_ref, chosen_ref, pick_sem)
    pick_copy.start()
    order_copy = pltpu.make_async_copy(order_ref, order_row, order_sem)
    order_copy.start()
    weight_copies = []
    for number, (start, size) in enumerate(tiles):
        copy = pltpu.make_async_copy(
            w_ref.at[:, pl.ds(start, size)], weight.at[:, pl.ds(start, size)], weight_sem.at[number]
        )
        copy.start(priority=1)
        weight_copies.append(copy)

    barrier = pltpu.get_barrier_semaphore()
    for partner in (first_up, first_down, second_up, second_down, pair):
        pl.semaphore_signal(barrier, inc=1, device_id={"vocab": partner}, device_id_type=MESH)

    own_copy.wait()
    pl.semaphore_wait(barrier, 5)

    started = []

    def push(src, dst, recv, to):
        copy = pltpu.make_async_remote_copy(
            src_ref=src, dst_ref=dst, send_sem=send_sem.at[len(started)], recv_sem=recv,
            device_id={"vocab": to}, device_id_type=MESH,
        )
        copy.start()
        started.append(copy)

    def wait_for(ref, sem):
        pltpu.make_async_remote_copy(
            src_ref=ref, dst_ref=ref, send_sem=send_sem.at[0], recv_sem=sem,
            device_id={"vocab": pair}, device_id_type=MESH,
        ).wait_recv()

    def arrived(rel, *pieces):
        for piece in pieces or range(PIECES[rel]):
            wait_for(block(rel, piece, PIECES[rel]), recv_sem.at[RECV[rel, piece]])

    def across(rel, to_rel, to, piece=0):
        count = PIECES[to_rel]
        push(block(rel, piece, count), block(to_rel, piece, count), recv_sem.at[RECV[to_rel, piece]], to)

    def along_second(rel, piece=0):
        across(rel, (rel[0], 3), second_up, piece)
        across(rel, (rel[0], 1), second_down, piece)

    def to_pair(rel, piece=0, count=1):
        push(block(rel, piece, count), block(rel, piece, count, 1), pair_sem.at[PLACE_HANDED[rel][0]], pair)

    def service(rel):
        arrived(rel)
        if rel == (2, 0):
            along_second(rel)
        elif rel[1] == 3:
            across(rel, (rel[0], 2), second_up, 0)
        elif rel[1] == 1:
            across(rel, (rel[0], 2), second_down, 1)
        to_pair(rel)

    def pair_arrived(chunk):
        handed = pl.ds(len(OWN[chunk]) * rows, len(HANDED[chunk]) * rows)
        wait_for(hidden.at[chunk, handed, :], pair_sem.at[chunk])

    across((0, 0), (3, 0), first_up, 0)
    across((0, 0), (1, 0), first_down, 1)
    along_second((0, 0))
    across((0, 0), (3, 0), first_up, 1)
    across((0, 0), (1, 0), first_down, 0)
    to_pair((0, 0))

    order_copy.wait()
    order = jnp.broadcast_to(order_row[...].astype(jnp.float32), (LANES, tokens))
    order = jnp.transpose(order).reshape(SHARDS, 2, rows // 2, LANES)
    order = jnp.concatenate([order[:, 0].reshape(-1, LANES), order[:, 1].reshape(-1, LANES)], axis=0)
    lanes = lax.broadcasted_iota(jnp.int32, (tokens, LANES), 1).astype(jnp.float32)
    for start in range(0, tokens, LANES):
        perm[:, pl.ds(start, LANES)] = jnp.where(order == lanes + start, 1.0, 0.0).astype(jnp.bfloat16)
    pick_copy.wait()
    for start in range(0, tokens, LANES):
        places = chosen_ref[:, pl.ds(start, LANES)] - me * width
        places = jnp.transpose(jnp.concatenate([places, places], axis=0))
        low[pl.ds(start, LANES), :] = places & (LANES - 1)
        high[pl.ds(start, LANES), :] = places >> 7

    for turn in (0, 1):
        for rel, half, on in (((3, 0), turn, first_up), ((1, 0), 1 - turn, first_down)):
            arrived(rel, half)
            if turn == 0:
                across(rel, (2, 0), on, half)
            to_pair(rel, half, 2)
            along_second(rel, half)
    service((0, 1))
    service((0, 3))

    services = {
        (0, 2): ((2, 0),), (0, 3): ((3, 3), (3, 1)), (0, 4): ((1, 1), (1, 3)),
        (1, 1): ((0, 2), (2, 1), (2, 3)), (2, 1): ((3, 2), (1, 2)), (2, 2): ((2, 2),),
    }

    def positions(chunk):
        spots = [at(*rel, core) for rel in OWN[chunk]] + [at(*rel, 1 - core) for rel in HANDED[chunk]]
        return [pl.multiple_of(spot * rows, rows) for spot in spots]

    def digest(chunk, number, spots):
        start, size = tiles[number]
        first = start // LANES
        part = pl.ds(0, COUNTS[chunk] * rows)
        values = [logits[part, pl.ds(start + LANES * k, LANES)] for k in range(size // LANES)]
        best = functools.reduce(jnp.maximum, values)
        if number == 0:
            total = jnp.zeros_like(best)
            chosen = jnp.zeros_like(best)
        else:
            old = top[part, :]
            best = jnp.maximum(best, old)
            total = mass[part, :] * jnp.exp(old - best)
            chosen = found[part, :]
        lane = jnp.concatenate([low[pl.ds(spot, rows), :] for spot in spots], axis=0)
        tile = jnp.concatenate([high[pl.ds(spot, rows), :] for spot in spots], axis=0)
        for k, value in enumerate(values):
            total = total + jnp.exp(value - best)
            taken = jnp.take_along_axis(value, lane, axis=1, mode="promise_in_bounds")
            chosen = jnp.where(tile == first + k, taken, chosen)
        top[part, :] = best
        mass[part, :] = total
        found[part, :] = chosen

    def finish(chunk, spots):
        digest(chunk, len(tiles) - 1, spots)
        part = pl.ds(0, COUNTS[chunk] * rows)
        best = top[part, :]
        peak = jnp.max(best, axis=1, keepdims=True)
        lse = peak + jnp.log(jnp.sum(mass[part, :] * jnp.exp(best - peak), axis=1, keepdims=True))
        lane = lax.broadcasted_iota(jnp.int32, best.shape, 1)
        rest = jnp.where(lane < picks, found[part, :], lse)
        parts = []
        for _ in range(2):
            part = rest.astype(jnp.bfloat16)
            rest = rest - part.astype(jnp.float32)
            parts.append(part)
        parts = jnp.concatenate(parts, axis=1)
        for k, spot in enumerate(spots):
            pieces[pl.ds(spot, rows), :] = parts[k * rows : (k + 1) * rows]

    for chunk in range(4):
        pair_arrived(chunk)
        if chunk == 0:
            for copy in weight_copies:
                copy.wait()
        for number, (start, size) in enumerate(tiles):
            part = pl.ds(0, COUNTS[chunk] * rows)
            logits[part, pl.ds(start, size)] = jnp.dot(
                hidden[chunk, part, :], weight[:, pl.ds(start, size)], preferred_element_type=jnp.float32
            )
            if number > 0:
                digest(chunk, number - 1, positions(chunk))
            elif chunk > 0:
                finish(chunk - 1, positions(chunk - 1))
            for rel in services.get((chunk, number), ()):
                service(rel)
    finish(3, positions(3))

    parts = jnp.dot(perm[...], pieces[...], preferred_element_type=jnp.float32)
    ordered = parts[:, :LANES] + parts[:, LANES:]
    upper, lower = ordered[: tokens // 2], ordered[tokens // 2 :]
    lane = lax.broadcasted_iota(jnp.int32, upper.shape, 1)
    outbox[...] = jnp.where(lane < picks, upper, pltpu.roll(lower, picks, 1)).reshape(outbox.shape)
    step = lax.broadcasted_iota(jnp.int32, upper.shape, 0) % (rows // 2)
    sums = jnp.where(lane == picks + step, upper, 0.0) + jnp.where(lane == picks + rows // 2 + step, lower, 0.0)
    for shard in range(SHARDS):
        part = sums[shard * (rows // 2) : (shard + 1) * (rows // 2)]
        sums_out[shard] = jnp.sum(part, axis=0, keepdims=True)

    for number, (dx, dz, dc) in enumerate(OTHERS):
        owner = flat(x + dx, z + dz, (core + dc) % 2)
        for source, target, sends, receives in (
            (outbox, inbox, out_sem, in_sem), (sums_out, sums_in, sums_out_sem, sums_in_sem)
        ):
            pltpu.make_async_remote_copy(
                src_ref=source.at[owner], dst_ref=target.at[number], send_sem=sends, recv_sem=receives,
                device_id={"vocab": owner}, device_id_type=MESH,
            ).start()
    for copy in started:
        copy.wait_send()

    def exchanged(target, sends, receives):
        return pltpu.make_async_remote_copy(
            src_ref=target, dst_ref=target, send_sem=sends, recv_sem=receives,
            device_id={"vocab": pair}, device_id_type=MESH,
        )

    picks_moved = exchanged(inbox, out_sem, in_sem)
    sums_moved = exchanged(sums_in, sums_out_sem, sums_in_sem)
    sums_moved.wait_recv()
    own_sum = sums_out[me]
    peak = jnp.maximum(jnp.max(sums_in[...], axis=0), own_sum)
    total = jnp.sum(jnp.exp(sums_in[...] - peak[None]), axis=0) + jnp.exp(own_sum - peak)
    total = peak + jnp.log(total)
    total_ref[...] = total[:, picks : picks + rows]
    lane = lax.broadcasted_iota(jnp.int32, (rows // 2, LANES), 1)
    step = lax.broadcasted_iota(jnp.int32, (rows // 2, LANES), 0)
    spread = jnp.broadcast_to(total, (rows // 2, LANES))
    first = jnp.sum(jnp.where(lane == picks + step, spread, 0.0), axis=1, keepdims=True)
    second = jnp.sum(jnp.where(lane == picks + rows // 2 + step, spread, 0.0), axis=1, keepdims=True)
    picks_moved.wait_recv()
    summed = jnp.sum(inbox[...], axis=0) + outbox[me] - jnp.where(lane < picks, first, second)
    logp_ref[pl.ds(0, rows // 2), :] = summed[:, :picks]
    logp_ref[pl.ds(rows // 2, rows // 2), :] = pltpu.roll(summed, picks, 1)[:, :picks]
    sums_moved.wait_send()
    picks_moved.wait_send()


def local(hidden_states, head_weight, pick_index, owner_order):
    rows, depth = hidden_states.shape
    width = head_weight.shape[1]
    tokens, picks = pick_index.shape
    chunk_rows = max(COUNTS) * rows
    tile_count = -(-width // TILE)
    operands = (hidden_states, head_weight, pick_index.T, owner_order.reshape(1, tokens))
    logp, total = pl.pallas_call(
        kernel,
        out_shape=(
            jax.ShapeDtypeStruct((rows, picks), jnp.float32),
            jax.ShapeDtypeStruct((1, rows), jnp.float32),
        ),
        in_specs=[
            pl.BlockSpec(memory_space=pltpu.HBM),
            pl.BlockSpec(memory_space=pltpu.HBM),
            pl.BlockSpec(memory_space=pltpu.HBM),
            pl.BlockSpec(memory_space=pltpu.HBM),
        ],
        out_specs=(pl.BlockSpec(memory_space=pltpu.VMEM), pl.BlockSpec(memory_space=pltpu.VMEM)),
        scratch_shapes=[
            pltpu.VMEM((4, chunk_rows, depth), jnp.bfloat16),
            pltpu.VMEM((depth, width), jnp.bfloat16),
            pltpu.VMEM((chunk_rows, width), jnp.float32),
            pltpu.VMEM((chunk_rows, LANES), jnp.float32),
            pltpu.VMEM((chunk_rows, LANES), jnp.float32),
            pltpu.VMEM((chunk_rows, LANES), jnp.float32),
            pltpu.VMEM((picks, tokens), jnp.int32),
            pltpu.VMEM((1, tokens), jnp.int32),
            pltpu.VMEM((tokens, LANES), jnp.int32),
            pltpu.VMEM((tokens, LANES), jnp.int32),
            pltpu.VMEM((tokens, 2 * LANES), jnp.bfloat16),
            pltpu.VMEM((tokens, tokens), jnp.bfloat16),
            pltpu.VMEM((SHARDS, rows // 2, LANES), jnp.float32),
            pltpu.VMEM((SHARDS - 1, rows // 2, LANES), jnp.float32),
            pltpu.VMEM((SHARDS, 1, LANES), jnp.float32),
            pltpu.VMEM((SHARDS - 1, 1, LANES), jnp.float32),
            pltpu.SemaphoreType.DMA,
            pltpu.SemaphoreType.DMA,
            pltpu.SemaphoreType.DMA,
            pltpu.SemaphoreType.DMA((tile_count,)),
            pltpu.SemaphoreType.DMA((SENDS,)),
            pltpu.SemaphoreType.DMA((len(RECV),)),
            pltpu.SemaphoreType.DMA((4,)),
            pltpu.SemaphoreType.DMA,
            pltpu.SemaphoreType.DMA,
            pltpu.SemaphoreType.DMA,
            pltpu.SemaphoreType.DMA,
        ],
        compiler_params=pltpu.CompilerParams(
            collective_id=0, has_side_effects=True, vmem_limit_bytes=48 * 1024 * 1024
        ),
    )(*(pltpu.with_memory_space_constraint(a, pltpu.HBM) for a in operands))
    return logp, total.reshape(rows)


def solution(mesh):
    in_specs = (P(("group", "vocab"), None), P(None, "vocab"), P("group", None), P("group"))
    out_specs = (P(("group", "vocab"), None), P(("group", "vocab")))
    return jax.shard_map(local, mesh=mesh, in_specs=in_specs, out_specs=out_specs, check_vma=False)
```
